8 devices in a mesh: fsdp: 8 (over z, y, x, core).
Axes of the slice: x: 2, y: 2, z: 1, core: 2. Of those that a mesh axis runs over, the one named last changes fastest.
Arguments:
- resid_in: bfloat16 [16, 730, 1280], P('fsdp')
- grad_out: bfloat16 [16, 730, 1280], P('fsdp')
- ln1_gain: float32 [1280], P('fsdp')
- ln1_bias: float32 [1280], P('fsdp')
- qkv_weight: float32 [1280, 3840], P('fsdp')
- qkv_bias: float32 [3840], P('fsdp')
- out_weight: float32 [1280, 1280], P('fsdp')
- out_bias: float32 [1280], P('fsdp')
- ln2_gain: float32 [1280], P('fsdp')
- ln2_bias: float32 [1280], P('fsdp')
- fc_weight: float32 [1280, 5120], P('fsdp')
- fc_bias: float32 [5120], P('fsdp')
- proj_weight: float32 [5120, 1280], P('fsdp')
- proj_bias: float32 [1280], P('fsdp')
Outputs:
- output 1: bfloat16 [16, 730, 1280], P('fsdp')
- output 2: bfloat16 [16, 730, 1280], P('fsdp')
- output 3: float32 [1280], P('fsdp')
- output 4: float32 [1280], P('fsdp')
- output 5: float32 [1280, 3840], P('fsdp')
- output 6: float32 [3840], P('fsdp')
- output 7: float32 [1280, 1280], P('fsdp')
- output 8: float32 [1280], P('fsdp')
- output 9: float32 [1280], P('fsdp')
- output 10: float32 [1280], P('fsdp')
- output 11: float32 [1280, 5120], P('fsdp')
- output 12: float32 [5120], P('fsdp')
- output 13: float32 [5120, 1280], P('fsdp')
- output 14: float32 [1280], P('fsdp')
All inputs are finite; a program needn't handle non-finite values.
Results may differ from the reference program's by a relative error of at most 0.02.
Values are sent between devices in bfloat16 or wider.
A program may use at most 1 GiB of HBM per device.

```python
import jax
import jax.numpy as jnp
from jax import lax

WIDTH = 1280
FFN = 5120
HEADS = 16
PATCHES = 729
BATCH = 16

SEQ = PATCHES + 1
HEAD_DIM = WIDTH // HEADS
LN_EPS = 1e-5


def setup_inputs(seed: int = 0) -> dict:
    keys = jax.random.split(jax.random.key(seed), 14)

    def normal(key_index, shape, scale):
        return jax.random.normal(keys[key_index], shape, jnp.float32) * scale

    return {
        "resid_in": normal(0, (BATCH, SEQ, WIDTH), 1.0).astype(jnp.bfloat16),
        "grad_out": normal(1, (BATCH, SEQ, WIDTH), 1.0).astype(jnp.bfloat16),
        "ln1_gain": 1.0 + normal(2, (WIDTH,), 0.6),
        "ln1_bias": normal(3, (WIDTH,), 1.0),
        "qkv_weight": normal(4, (WIDTH, 3 * WIDTH), WIDTH ** -0.5),
        "qkv_bias": normal(5, (3 * WIDTH,), 1.0),
        "out_weight": normal(6, (WIDTH, WIDTH), WIDTH ** -0.5),
        "out_bias": normal(7, (WIDTH,), 1.0),
        "ln2_gain": 1.0 + normal(8, (WIDTH,), 0.6),
        "ln2_bias": normal(9, (WIDTH,), 1.0),
        "fc_weight": normal(10, (WIDTH, FFN), WIDTH ** -0.5),
        "fc_bias": normal(11, (FFN,), 1.0),
        "proj_weight": normal(12, (FFN, WIDTH), FFN ** -0.5),
        "proj_bias": normal(13, (WIDTH,), 1.0),
    }


def layer_norm(values, gain, bias):
    mean_val = jnp.mean(values, axis=-1, keepdims=True)
    centered = values - mean_val
    variance = jnp.mean(centered * centered, axis=-1, keepdims=True)
    return centered * lax.rsqrt(variance + LN_EPS) * gain + bias


def layer_forward(params, tokens):
    (ln1_gain, ln1_bias, qkv_weight, qkv_bias, out_weight, out_bias,
     ln2_gain, ln2_bias, fc_weight, fc_bias, proj_weight, proj_bias) = [param.astype(jnp.bfloat16) for param in params]
    resid = tokens.astype(jnp.float32)
    normed_one = layer_norm(resid, ln1_gain, ln1_bias).astype(jnp.bfloat16)
    qkv_vals = (jnp.dot(normed_one, qkv_weight, preferred_element_type=jnp.float32) + qkv_bias).astype(jnp.bfloat16)
    qkv_vals = qkv_vals.reshape(SEQ, 3, HEADS, HEAD_DIM).astype(jnp.float32)
    scores = jnp.einsum("qhd,khd->hqk", qkv_vals[:, 0], qkv_vals[:, 1]) * (HEAD_DIM ** -0.5)
    attn_probs = jax.nn.softmax(scores, axis=-1).astype(jnp.bfloat16).astype(jnp.float32)
    mixed = jnp.einsum("hqk,khd->qhd", attn_probs, qkv_vals[:, 2]).astype(jnp.bfloat16).reshape(SEQ, WIDTH)
    middle = (resid + jnp.dot(mixed, out_weight, preferred_element_type=jnp.float32) + out_bias).astype(jnp.bfloat16)
    middle_wide = middle.astype(jnp.float32)
    normed_two = layer_norm(middle_wide, ln2_gain, ln2_bias).astype(jnp.bfloat16)
    pre_act = jnp.dot(normed_two, fc_weight, preferred_element_type=jnp.float32) + fc_bias
    hidden = jax.nn.gelu(pre_act, approximate=False).astype(jnp.bfloat16)
    return (middle_wide + jnp.dot(hidden, proj_weight, preferred_element_type=jnp.float32) + proj_bias).astype(jnp.bfloat16)


def reference(resid_in, grad_out, ln1_gain, ln1_bias, qkv_weight, qkv_bias, out_weight, out_bias,
              ln2_gain, ln2_bias, fc_weight, fc_bias, proj_weight, proj_bias):
    params = (ln1_gain, ln1_bias, qkv_weight, qkv_bias, out_weight, out_bias,
              ln2_gain, ln2_bias, fc_weight, fc_bias, proj_weight, proj_bias)

    def per_image(grad_sum, pair):
        tokens, cotangent = pair
        image_out, pullback = jax.vjp(layer_forward, params, tokens)
        param_grads, token_grad = pullback(cotangent)
        grad_sum = jax.tree.map(lambda total, fresh: total + fresh, grad_sum, param_grads)
        return grad_sum, (image_out, token_grad)

    start_sum = jax.tree.map(jnp.zeros_like, params)
    grad_sum, (resid_out, grad_in) = lax.scan(per_image, start_sum, (resid_in, grad_out))
    (grad_ln1_gain, grad_ln1_bias, grad_qkv_weight, grad_qkv_bias, grad_out_weight, grad_out_bias,
     grad_ln2_gain, grad_ln2_bias, grad_fc_weight, grad_fc_bias, grad_proj_weight, grad_proj_bias) = grad_sum
    return (resid_out, grad_in, grad_ln1_gain, grad_ln1_bias, grad_qkv_weight, grad_qkv_bias,
            grad_out_weight, grad_out_bias, grad_ln2_gain, grad_ln2_bias, grad_fc_weight, grad_fc_bias,
            grad_proj_weight, grad_proj_bias)
```

```python
import functools
import math

import jax
import jax.numpy as jnp
from jax import lax
from jax.experimental import pallas as pl
from jax.experimental.pallas import tpu as pltpu
from jax.sharding import PartitionSpec as P

HEADS = 16
HEAD_DIM = 80
GROUP = 8
GROUP_COLS = GROUP * HEAD_DIM
SCALE = HEAD_DIM ** -0.5
LOG2E = math.log2(math.e)
LN_EPS = 1e-5
F32 = jnp.float32
BF16 = jnp.bfloat16
VMEM_LIMIT = 60 * 2 ** 20


def dot(lhs, rhs, lhs_dim, rhs_dim):
    return lax.dot_general(lhs, rhs, (((lhs_dim,), (rhs_dim,)), ((), ())), preferred_element_type=F32)


def attn_fwd_kernel(q_ref, k_ref, v_ref, o_ref, lse_ref):
    for head in range(GROUP):
        cols = slice(head * HEAD_DIM, (head + 1) * HEAD_DIM)
        scores = dot(k_ref[0, :, cols], q_ref[0, :, cols], 1, 1)
        top = jnp.max(scores, axis=0, keepdims=True)
        expo = jnp.exp2((scores - top) * (SCALE * LOG2E))
        total = jnp.sum(expo, axis=0, keepdims=True)
        probs = (expo * (1.0 / total)).astype(BF16)
        o_ref[0, :, cols] = dot(probs, v_ref[0, :, cols], 0, 0).astype(BF16)
        lse_ref[0, 0, head:head + 1, :] = top * (SCALE * LOG2E) + jnp.log2(total)


def attn_bwd_kernel(q_ref, k_ref, v_ref, do_ref, lse_ref, dq_ref, dk_ref, dv_ref):
    for head in range(GROUP):
        cols = slice(head * HEAD_DIM, (head + 1) * HEAD_DIM)
        q, k, v, do = q_ref[0, :, cols], k_ref[0, :, cols], v_ref[0, :, cols], do_ref[0, :, cols]
        scores = dot(k, q, 1, 1)
        probs = jnp.exp2(scores * (SCALE * LOG2E) - lse_ref[0, 0, head:head + 1, :])
        grad_probs = dot(v, do, 1, 1)
        dv_ref[0, :, cols] = dot(probs.astype(BF16), do, 1, 0).astype(BF16)
        delta = jnp.sum(probs * grad_probs, axis=0, keepdims=True)
        grad_scores = (probs * ((grad_probs - delta) * SCALE)).astype(BF16)
        dk_ref[0, :, cols] = dot(grad_scores, q, 1, 0).astype(BF16)
        dq_ref[0, :, cols] = dot(grad_scores, k, 0, 0).astype(BF16)


def attn_specs(qkv):
    images, seq_len, _ = qkv.shape
    groups = qkv.shape[2] // 3 // GROUP_COLS

    def cols(part):
        return pl.BlockSpec((1, seq_len, GROUP_COLS), lambda b, g: (b, 0, part * groups + g))

    lse = pl.BlockSpec((1, 1, GROUP, seq_len), lambda b, g: (b, g, 0, 0))
    return images, seq_len, groups, cols, lse


def attn_fwd(qkv):
    images, seq_len, groups, cols, lse = attn_specs(qkv)
    width = groups * GROUP_COLS
    return pl.pallas_call(
        attn_fwd_kernel, grid=(images, groups), name="attn_fwd",
        in_specs=[cols(0), cols(1), cols(2)], out_specs=[cols(0), lse],
        out_shape=[jax.ShapeDtypeStruct((images, seq_len, width), BF16),
                   jax.ShapeDtypeStruct((images, groups, GROUP, seq_len), F32)],
        cost_estimate=pl.CostEstimate(flops=30 * 10 ** 9, bytes_accessed=16 * 10 ** 6, transcendentals=0),
        compiler_params=pltpu.CompilerParams(vmem_limit_bytes=VMEM_LIMIT))(qkv, qkv, qkv)


def attn_bwd(qkv, grad_mixed, lse_vals):
    images, seq_len, groups, cols, lse = attn_specs(qkv)
    width = groups * GROUP_COLS
    return pl.pallas_call(
        attn_bwd_kernel, grid=(images, groups), name="attn_bwd",
        in_specs=[cols(0), cols(1), cols(2), cols(0), lse], out_specs=[cols(0)] * 3,
        out_shape=[jax.ShapeDtypeStruct((images, seq_len, width), BF16)] * 3,
        cost_estimate=pl.CostEstimate(flops=50 * 10 ** 9, bytes_accessed=30 * 10 ** 6, transcendentals=0),
        compiler_params=pltpu.CompilerParams(vmem_limit_bytes=VMEM_LIMIT))(qkv, qkv, qkv, grad_mixed, lse_vals)


def fc_gelu_kernel(x_ref, w_ref, b_ref, h_ref, slope_ref):
    for image in range(x_ref.shape[0]):
        pre = dot(x_ref[image], w_ref[...], 1, 0) + b_ref[...]
        cdf = 0.5 + 0.5 * lax.erf(pre * (0.5 ** 0.5))
        pdf = jnp.exp2(pre * pre * (-0.5 * LOG2E)) * ((2.0 * math.pi) ** -0.5)
        h_ref[image] = (pre * cdf).astype(BF16)
        slope_ref[image] = cdf + pre * pdf


def fc_gelu(normed, weight, bias, tile=512):
    images, seq_len, width = normed.shape
    ffn = weight.shape[1]
    out = pl.BlockSpec((images, seq_len, tile), lambda j: (0, 0, j))
    return pl.pallas_call(
        fc_gelu_kernel, grid=(ffn // tile,), name="fc_gelu",
        in_specs=[pl.BlockSpec((images, seq_len, width), lambda j: (0, 0, 0)),
                  pl.BlockSpec((width, tile), lambda j: (0, j)), pl.BlockSpec((1, tile), lambda j: (0, j))],
        out_specs=[out, out],
        out_shape=[jax.ShapeDtypeStruct((images, seq_len, ffn), BF16),
                   jax.ShapeDtypeStruct((images, seq_len, ffn), F32)],
        cost_estimate=pl.CostEstimate(flops=30 * 10 ** 9, bytes_accessed=60 * 10 ** 6, transcendentals=0),
        compiler_params=pltpu.CompilerParams(vmem_limit_bytes=VMEM_LIMIT))(normed, weight, bias.reshape(1, ffn))


def layer_norm_fwd(values, gain, bias):
    mean_val = jnp.mean(values, axis=-1, keepdims=True)
    centered = values - mean_val
    inv_std = lax.rsqrt(jnp.mean(centered * centered, axis=-1, keepdims=True) + LN_EPS)
    x_hat = centered * inv_std
    return x_hat * gain + bias, x_hat, inv_std


def layer_norm_bwd(grad_norm, x_hat, inv_std, gain):
    grad_hat = grad_norm * gain
    grad_vals = inv_std * (grad_hat - jnp.mean(grad_hat, axis=-1, keepdims=True)
                           - x_hat * jnp.mean(grad_hat * x_hat, axis=-1, keepdims=True))
    return grad_vals, jnp.sum(grad_norm * x_hat, axis=(0, 1)), jnp.sum(grad_norm, axis=(0, 1))


def einsum(spec, lhs, rhs):
    return jnp.einsum(spec, lhs, rhs, preferred_element_type=F32)


def solution(mesh):
    specs = (P("fsdp"),) * 14
    n = mesh.shape["fsdp"]

    def gather(shard):
        return lax.all_gather(shard.astype(BF16), "fsdp", axis=0, tiled=True)

    def scatter(grad):
        return lax.psum_scatter(grad, "fsdp", scatter_dimension=0, tiled=True)

    def device_step(resid_in, grad_out, ln1_gain, ln1_bias, qkv_weight, qkv_bias, out_weight, out_bias,
                    ln2_gain, ln2_bias, fc_weight, fc_bias, proj_weight, proj_bias):
        vectors = (ln1_gain, ln1_bias, qkv_bias, out_bias, ln2_gain, ln2_bias, fc_bias, proj_bias)
        packed = jnp.concatenate(vectors).astype(BF16)
        packed = lax.all_gather(packed, "fsdp", axis=0)
        full, at = [], 0
        for vec in vectors:
            full.append(packed[:, at:at + vec.shape[0]].reshape(-1))
            at += vec.shape[0]
        ln1_gain, ln1_bias, qkv_bias, out_bias, ln2_gain, ln2_bias, fc_bias, proj_bias = [f.astype(F32) for f in full]
        qkv_weight, out_weight, fc_weight, proj_weight = [gather(w) for w in (qkv_weight, out_weight, fc_weight, proj_weight)]

        resid = resid_in.astype(F32)
        normed, hat_one, inv_one = layer_norm_fwd(resid, ln1_gain, ln1_bias)
        normed_one = normed.astype(BF16)
        qkv = (einsum("bsw,wk->bsk", normed_one, qkv_weight) + qkv_bias).astype(BF16)
        mixed, lse = attn_fwd(qkv)
        middle = (resid + einsum("bsw,wv->bsv", mixed, out_weight) + out_bias).astype(BF16)
        middle_wide = middle.astype(F32)
        normed, hat_two, inv_two = layer_norm_fwd(middle_wide, ln2_gain, ln2_bias)
        normed_two = normed.astype(BF16)
        hidden, slope = fc_gelu(normed_two, fc_weight, fc_bias)
        resid_out = (middle_wide + einsum("bsf,fw->bsw", hidden, proj_weight) + proj_bias).astype(BF16)

        grad_wide = grad_out.astype(F32)
        d_proj_weight = scatter(einsum("bsf,bsw->fw", hidden, grad_out))
        d_proj_bias = jnp.sum(grad_wide, axis=(0, 1))
        grad_pre = einsum("bsw,fw->bsf", grad_out, proj_weight) * slope
        grad_pre_low = grad_pre.astype(BF16)
        d_fc_bias = jnp.sum(grad_pre, axis=(0, 1))
        d_fc_weight = scatter(einsum("bsw,bsf->wf", normed_two, grad_pre_low))
        grad_norm = einsum("bsf,wf->bsw", grad_pre_low, fc_weight)
        grad_ln, d_ln2_gain, d_ln2_bias = layer_norm_bwd(grad_norm, hat_two, inv_two, ln2_gain)
        grad_middle = grad_wide + grad_ln
        grad_middle_low = grad_middle.astype(BF16)
        d_out_weight = scatter(einsum("bsw,bsv->wv", mixed, grad_middle_low))
        d_out_bias = jnp.sum(grad_middle, axis=(0, 1))
        grad_mixed = einsum("bsv,wv->bsw", grad_middle_low, out_weight).astype(BF16)
        parts = attn_bwd(qkv, grad_mixed, lse)
        grad_qkv = jnp.concatenate(parts, axis=-1)
        d_qkv_weight = scatter(einsum("bsw,bsk->wk", normed_one, grad_qkv))
        d_qkv_bias = jnp.sum(grad_qkv.astype(F32), axis=(0, 1))
        grad_norm = einsum("bsk,wk->bsw", grad_qkv, qkv_weight)
        grad_ln, d_ln1_gain, d_ln1_bias = layer_norm_bwd(grad_norm, hat_one, inv_one, ln1_gain)
        grad_in = (grad_middle + grad_ln).astype(BF16)

        small = (d_ln1_gain, d_ln1_bias, d_qkv_bias, d_out_bias, d_ln2_gain, d_ln2_bias, d_fc_bias, d_proj_bias)
        summed = lax.psum_scatter(jnp.concatenate([s.reshape(n, -1) for s in small], axis=1), "fsdp",
                                  scatter_dimension=0, tiled=True).reshape(-1)
        shards, at = [], 0
        for vec in small:
            shards.append(summed[at:at + vec.shape[0] // n])
            at += vec.shape[0] // n
        (d_ln1_gain, d_ln1_bias, d_qkv_bias, d_out_bias, d_ln2_gain, d_ln2_bias, d_fc_bias, d_proj_bias) = shards
        return (resid_out, grad_in, d_ln1_gain, d_ln1_bias, d_qkv_weight, d_qkv_bias, d_out_weight, d_out_bias,
                d_ln2_gain, d_ln2_bias, d_fc_weight, d_fc_bias, d_proj_weight, d_proj_bias)

    return jax.shard_map(device_step, mesh=mesh, in_specs=specs, out_specs=specs, check_vma=False)
```

```python
import functools
import math

import jax
import jax.numpy as jnp
from jax import lax
from jax.experimental import pallas as pl
from jax.experimental.pallas import tpu as pltpu
from jax.sharding import PartitionSpec as P

HEADS = 16
HEAD_DIM = 80
GROUP = 8
GROUP_COLS = GROUP * HEAD_DIM
ROWS = 640
CORE_BIT, X_BIT, Y_BIT = 1, 2, 4
SCALE = HEAD_DIM ** -0.5
LOG2E = math.log2(math.e)
LN_EPS = 1e-5
F32 = jnp.float32
BF16 = jnp.bfloat16
VMEM_LIMIT = 60 * 2 ** 20


def dot(lhs, rhs, lhs_dim, rhs_dim):
    return lax.dot_general(lhs, rhs, (((lhs_dim,), (rhs_dim,)), ((), ())), preferred_element_type=F32)


def attn_fwd_kernel(q_ref, k_ref, v_ref, o_ref, lse_ref):
    for head in range(GROUP):
        cols = slice(head * HEAD_DIM, (head + 1) * HEAD_DIM)
        scores = dot(k_ref[0, :, cols], q_ref[0, :, cols], 1, 1)
        top = jnp.max(scores, axis=0, keepdims=True)
        expo = jnp.exp2((scores - top) * (SCALE * LOG2E))
        total = jnp.sum(expo, axis=0, keepdims=True)
        probs = (expo * (1.0 / total)).astype(BF16)
        o_ref[0, :, cols] = dot(probs, v_ref[0, :, cols], 0, 0).astype(BF16)
        lse_ref[0, 0, head:head + 1, :] = top * (SCALE * LOG2E) + jnp.log2(total)


def attn_bwd_kernel(q_ref, k_ref, v_ref, do_ref, lse_ref, dqkv_ref, dbias_ref, dq_ref, dk_ref, dv_ref, sums_ref):
    for head in range(GROUP):
        cols = slice(head * HEAD_DIM, (head + 1) * HEAD_DIM)
        q, k, v, do = q_ref[0, :, cols], k_ref[0, :, cols], v_ref[0, :, cols], do_ref[0, :, cols]
        scores = dot(k, q, 1, 1)
        probs = jnp.exp2(scores * (SCALE * LOG2E) - lse_ref[0, 0, head:head + 1, :])
        grad_probs = dot(v, do, 1, 1)
        grad_v = dot(probs.astype(BF16), do, 1, 0)
        delta = jnp.sum(probs * grad_probs, axis=0, keepdims=True)
        grad_scores = (probs * ((grad_probs - delta) * SCALE)).astype(BF16)
        grad_k = dot(grad_scores, q, 1, 0)
        grad_q = dot(grad_scores, k, 0, 0)
        for part, (grad, ref) in enumerate(((grad_q, dq_ref), (grad_k, dk_ref), (grad_v, dv_ref))):
            ref[:, cols] = grad.astype(BF16)
            sums_ref[part, :, cols] = jnp.sum(grad, axis=0, keepdims=True)
    width = dqkv_ref.shape[2] // 3
    for part, ref in enumerate((dq_ref, dk_ref, dv_ref)):
        cols = pl.ds(pl.multiple_of(part * width + pl.program_id(1) * GROUP_COLS, 128), GROUP_COLS)
        dqkv_ref[0, :, cols] = ref[...]
        dbias_ref[0, :, cols] = sums_ref[part]


def attn_specs(qkv):
    images, seq_len, _ = qkv.shape
    groups = qkv.shape[2] // 3 // GROUP_COLS

    def cols(part):
        return pl.BlockSpec((1, seq_len, GROUP_COLS), lambda b, g: (b, 0, part * groups + g))

    lse = pl.BlockSpec((1, 1, GROUP, seq_len), lambda b, g: (b, g, 0, 0))
    return images, seq_len, groups, cols, lse


def attn_fwd(qkv):
    images, seq_len, groups, cols, lse = attn_specs(qkv)
    width = groups * GROUP_COLS
    return pl.pallas_call(
        attn_fwd_kernel, grid=(images, groups), name="attn_fwd",
        in_specs=[cols(0), cols(1), cols(2)], out_specs=[cols(0), lse],
        out_shape=[jax.ShapeDtypeStruct((images, seq_len, width), BF16),
                   jax.ShapeDtypeStruct((images, groups, GROUP, seq_len), F32)],
        cost_estimate=pl.CostEstimate(flops=30 * 10 ** 9, bytes_accessed=16 * 10 ** 6, transcendentals=0),
        compiler_params=pltpu.CompilerParams(vmem_limit_bytes=VMEM_LIMIT))(qkv, qkv, qkv)


def attn_bwd(qkv, grad_mixed, lse_vals):
    images, seq_len, groups, cols, lse = attn_specs(qkv)
    out_cols = qkv.shape[2]
    return pl.pallas_call(
        attn_bwd_kernel, grid=(images, groups), name="attn_bwd",
        in_specs=[cols(0), cols(1), cols(2), cols(0), lse],
        out_specs=[pl.BlockSpec((1, seq_len, out_cols), lambda b, g: (b, 0, 0)),
                   pl.BlockSpec((1, 1, out_cols), lambda b, g: (b, 0, 0))],
        out_shape=[jax.ShapeDtypeStruct((images, seq_len, out_cols), BF16),
                   jax.ShapeDtypeStruct((images, 1, out_cols), F32)],
        scratch_shapes=[pltpu.VMEM((seq_len, GROUP_COLS), BF16)] * 3 + [pltpu.VMEM((3, 1, GROUP_COLS), F32)],
        cost_estimate=pl.CostEstimate(flops=50 * 10 ** 9, bytes_accessed=30 * 10 ** 6, transcendentals=0),
        compiler_params=pltpu.CompilerParams(vmem_limit_bytes=VMEM_LIMIT))(qkv, qkv, qkv, grad_mixed, lse_vals)


def fc_gelu_kernel(x_ref, w_ref, b_ref, h_ref, slope_ref):
    for image in range(x_ref.shape[0]):
        pre = dot(x_ref[image], w_ref[...], 1, 0) + b_ref[...]
        cdf = 0.5 + 0.5 * lax.erf(pre * (0.5 ** 0.5))
        pdf = jnp.exp2(pre * pre * (-0.5 * LOG2E)) * ((2.0 * math.pi) ** -0.5)
        h_ref[image] = (pre * cdf).astype(BF16)
        slope_ref[image] = cdf + pre * pdf


def fc_gelu(normed, weight, bias, tile=512):
    images, seq_len, width = normed.shape
    ffn = weight.shape[1]
    out = pl.BlockSpec((images, seq_len, tile), lambda j: (0, 0, j))
    return pl.pallas_call(
        fc_gelu_kernel, grid=(ffn // tile,), name="fc_gelu",
        in_specs=[pl.BlockSpec((images, seq_len, width), lambda j: (0, 0, 0)),
                  pl.BlockSpec((width, tile), lambda j: (0, j)), pl.BlockSpec((1, tile), lambda j: (0, j))],
        out_specs=[out, out],
        out_shape=[jax.ShapeDtypeStruct((images, seq_len, ffn), BF16),
                   jax.ShapeDtypeStruct((images, seq_len, ffn), F32)],
        cost_estimate=pl.CostEstimate(flops=30 * 10 ** 9, bytes_accessed=60 * 10 ** 6, transcendentals=0),
        compiler_params=pltpu.CompilerParams(vmem_limit_bytes=VMEM_LIMIT))(normed, weight, bias.reshape(1, ffn))


def wgrad_tile(acts_ref, grad_ref):
    total = dot(acts_ref[0], grad_ref[0], 0, 0)
    for image in range(1, acts_ref.shape[0]):
        total += dot(acts_ref[image], grad_ref[image], 0, 0)
    return total


def send_kernel(pos, acts_ref, grad_ref, out_ref):
    out_ref[...] = wgrad_tile(acts_ref, grad_ref).astype(BF16).reshape(out_ref.shape)


def keep_kernel(pos, acts_ref, grad_ref, recv_ref, keep_a, keep_b, send_a, send_b, total, *, piece, by_rows):
    y, x = pos[0], pos[1]
    total[...] = wgrad_tile(acts_ref, grad_ref) + recv_ref[...].reshape(total.shape).astype(F32)
    step = pl.program_id(1)

    def put(to_a, row_y, row_x, rows, cols):
        mine = row_x == x if to_a else row_y == y
        keep, send, slot = (keep_a, send_a, row_y) if to_a else (keep_b, send_b, row_x)

        @pl.when(mine)
        def _():
            keep[slot] = total[rows, cols]

        @pl.when(jnp.logical_not(mine))
        def _():
            send[slot] = total[rows, cols].astype(BF16)

    if by_rows:
        half = total.shape[1] // 2
        put(True, step // 2, step % 2, slice(None), slice(0, half))
        put(False, step // 2, step % 2, slice(None), slice(half, 2 * half))
    else:
        for block in range(ROWS // piece):
            put(block % 2 == 0, step, block // 2, slice(block * piece, (block + 1) * piece), slice(None))


def wgrad_call(acts, grad, pos, recv, grid, acts_spec, grad_spec, tile, sent_shape, kept_block, kept_shape, piece, by_rows):
    images, seq_len, depth = acts.shape
    flops = images * seq_len * depth * grad.shape[2]
    if recv is None:
        kernel, outs, scratch, args = send_kernel, tile, [], ()
        shapes = jax.ShapeDtypeStruct(sent_shape, BF16)
        ins = [acts_spec, grad_spec]
    else:
        kernel = functools.partial(keep_kernel, piece=piece, by_rows=by_rows)
        outs, args, ins = [kept_block] * 4, (recv,), [acts_spec, grad_spec, tile]
        shapes = [jax.ShapeDtypeStruct(kept_shape, kind) for kind in (F32, F32, BF16, BF16)]
        scratch = [pltpu.VMEM(tile.block_shape[-2:], F32)]
    return pl.pallas_call(
        kernel, out_shape=shapes, name="wgrad_send" if recv is None else "wgrad_keep",
        grid_spec=pltpu.PrefetchScalarGridSpec(num_scalar_prefetch=1, grid=grid, in_specs=ins, out_specs=outs,
                                               scratch_shapes=scratch),
        cost_estimate=pl.CostEstimate(flops=flops, bytes_accessed=20 * 10 ** 6, transcendentals=0),
        compiler_params=pltpu.CompilerParams(vmem_limit_bytes=VMEM_LIMIT))(pos, acts, grad, *args)


def wgrad_cols(acts, grad, pos, tile_n, recv=None):
    images, seq_len, depth = acts.shape
    width = grad.shape[2] // 2
    blocks, piece = width // tile_n, depth // 8
    own = recv is not None
    return wgrad_call(
        acts, grad, pos, recv, (blocks, depth // ROWS),
        pl.BlockSpec((images, seq_len, ROWS), lambda j, i, p: (0, 0, i)),
        pl.BlockSpec((images, seq_len, tile_n), lambda j, i, p: (0, 0, (p[2] if own else 1 - p[2]) * blocks + j)),
        pl.BlockSpec((ROWS, tile_n), lambda j, i, p: (i, j)), (depth, width),
        pl.BlockSpec((2, piece, tile_n), lambda j, i, p: (0, 0, j)), (2, piece, width), piece, False)


def wgrad_rows(acts, grad, pos, recv=None):
    images, seq_len, _ = acts.shape
    width = grad.shape[2]
    own = recv is not None
    return wgrad_call(
        acts, grad, pos, recv, (1, 4),
        pl.BlockSpec((images, seq_len, ROWS), lambda j, i, p: (0, 0, 2 * i + (p[2] if own else 1 - p[2]))),
        pl.BlockSpec((images, seq_len, width), lambda j, i, p: (0, 0, 0)),
        pl.BlockSpec((1, ROWS, width), lambda j, i, p: (i, 0, 0)), (4, ROWS, width),
        pl.BlockSpec((2, ROWS, width // 2), lambda j, i, p: (0, 0, 0)), (2, ROWS, width // 2), ROWS, True)


def layer_norm_fwd(values, gain, bias):
    mean_val = jnp.mean(values, axis=-1, keepdims=True)
    centered = values - mean_val
    inv_std = lax.rsqrt(jnp.mean(centered * centered, axis=-1, keepdims=True) + LN_EPS)
    x_hat = centered * inv_std
    return x_hat * gain + bias, x_hat, inv_std


def layer_norm_bwd(grad_norm, x_hat, inv_std, gain):
    grad_hat = grad_norm * gain
    grad_vals = inv_std * (grad_hat - jnp.mean(grad_hat, axis=-1, keepdims=True)
                           - x_hat * jnp.mean(grad_hat * x_hat, axis=-1, keepdims=True))
    return grad_vals, jnp.sum(grad_norm * x_hat, axis=(0, 1)), jnp.sum(grad_norm, axis=(0, 1))


def einsum(spec, lhs, rhs):
    return jnp.einsum(spec, lhs, rhs, preferred_element_type=F32)


def flip(value, bit):
    return lax.ppermute(value, "fsdp", [(d, d ^ bit) for d in range(8)])


def pick(value, index):
    return lax.dynamic_index_in_dim(value, index, 0, keepdims=False).astype(F32)


def after(value, *done):
    return lax.optimization_barrier((value,) + done)[0]


def held(kept, *done):
    keep_a, keep_b = lax.optimization_barrier((kept[0], kept[1]) + done)[:2]
    return keep_a, keep_b, kept[2], kept[3]


def cross_first(kept, pos):
    keep_a, keep_b, send_a, send_b = kept
    y, x = pos[0], pos[1]
    recv_a, recv_b = flip(send_a, X_BIT), flip(send_b, Y_BIT)
    next_a = (pick(keep_a, 1 - y) + pick(recv_a, 1 - y)).astype(BF16)
    next_b = (pick(keep_b, 1 - x) + pick(recv_b, 1 - x)).astype(BF16)
    return next_a, next_b, keep_a, keep_b, recv_a, recv_b


def cross_second(state, pos):
    next_a, next_b, keep_a, keep_b, recv_a, recv_b = state
    y, x = pos[0], pos[1]
    last_a, last_b = flip(next_a, Y_BIT), flip(next_b, X_BIT)
    return (pick(keep_a, y) + pick(recv_a, y) + last_a.astype(F32),
            pick(keep_b, x) + pick(recv_b, x) + last_b.astype(F32))


def finish_cols(sum_a, sum_b, pos):
    core = pos[2]
    mine = jnp.where(core == 0, sum_a, sum_b)
    other = flip(jnp.where(core == 0, sum_b, sum_a), CORE_BIT)
    return jnp.where(core == 0, jnp.concatenate([mine, other], axis=1), jnp.concatenate([other, mine], axis=1))


def sum_kernel(n, in_ref, out_ref, recv, send_sem, recv_sem):
    me = lax.axis_index("fsdp")
    barrier = pltpu.get_barrier_semaphore()
    peers = [lax.rem(me + step, n) for step in range(1, n)]
    for peer in peers:
        pl.semaphore_signal(barrier, inc=1, device_id=(peer,), device_id_type=pl.DeviceIdType.MESH)
    pl.semaphore_wait(barrier, n - 1)
    copies = []
    for step, peer in enumerate(peers):
        copies.append(pltpu.make_async_remote_copy(
            src_ref=in_ref.at[peer], dst_ref=recv.at[step], send_sem=send_sem.at[step], recv_sem=recv_sem.at[step],
            device_id=(peer,), device_id_type=pl.DeviceIdType.MESH))
        copies[-1].start()
    total = in_ref[me]
    for step, copy in enumerate(copies):
        copy.wait()
        total += recv[step]
    out_ref[...] = total


def sum_scatter(values):
    n, rows, cols = values.shape
    return pl.pallas_call(
        functools.partial(sum_kernel, n), name="sum_scatter",
        in_specs=[pl.BlockSpec(memory_space=pltpu.VMEM)], out_specs=pl.BlockSpec(memory_space=pltpu.VMEM),
        out_shape=jax.ShapeDtypeStruct((rows, cols), F32),
        scratch_shapes=[pltpu.VMEM((n - 1, rows, cols), F32), pltpu.SemaphoreType.DMA((n - 1,)),
                        pltpu.SemaphoreType.DMA((n - 1,))],
        cost_estimate=pl.CostEstimate(flops=4 * 10 ** 9, bytes_accessed=10 ** 6, transcendentals=0),
        compiler_params=pltpu.CompilerParams(collective_id=0, has_side_effects=True))(values)


def solution(mesh):
    specs = (P("fsdp"),) * 14
    n = mesh.shape["fsdp"]

    def gather(shard):
        return lax.all_gather(shard.astype(BF16), "fsdp", axis=0, tiled=True)

    def device_step(resid_in, grad_out, ln1_gain, ln1_bias, qkv_weight, qkv_bias, out_weight, out_bias,
                    ln2_gain, ln2_bias, fc_weight, fc_bias, proj_weight, proj_bias):
        vectors = (ln1_gain, ln1_bias, qkv_bias, out_bias, ln2_gain, ln2_bias, fc_bias, proj_bias)
        packed = jnp.concatenate(vectors).astype(BF16)
        packed = lax.all_gather(packed, "fsdp", axis=0)
        full, at = [], 0
        for vec in vectors:
            full.append(packed[:, at:at + vec.shape[0]].reshape(-1))
            at += vec.shape[0]
        ln1_gain, ln1_bias, qkv_bias, out_bias, ln2_gain, ln2_bias, fc_bias, proj_bias = [f.astype(F32) for f in full]
        qkv_weight, out_weight, fc_weight, proj_weight = [gather(w) for w in (qkv_weight, out_weight, fc_weight, proj_weight)]

        resid = resid_in.astype(F32)
        normed, hat_one, inv_one = layer_norm_fwd(resid, ln1_gain, ln1_bias)
        normed_one = normed.astype(BF16)
        qkv = (einsum("bsw,wk->bsk", normed_one, qkv_weight) + qkv_bias).astype(BF16)
        mixed, lse = attn_fwd(qkv)
        middle = (resid + einsum("bsw,wv->bsv", mixed, out_weight) + out_bias).astype(BF16)
        middle_wide = middle.astype(F32)
        normed, hat_two, inv_two = layer_norm_fwd(middle_wide, ln2_gain, ln2_bias)
        normed_two = normed.astype(BF16)
        hidden, slope = fc_gelu(normed_two, fc_weight, fc_bias)

        device = lax.axis_index("fsdp")
        pos = jnp.stack([device // Y_BIT, (device // X_BIT) % 2, device % 2]).astype(jnp.int32)
        grad_wide = grad_out.astype(F32)
        d_proj_bias = jnp.sum(grad_wide, axis=(0, 1))
        proj_sent = flip(wgrad_rows(hidden, grad_out, pos), CORE_BIT)
        proj_kept = wgrad_rows(hidden, grad_out, pos, proj_sent)
        grad_pre = einsum("bsw,fw->bsf", after(grad_out, proj_kept[2], proj_kept[3]), proj_weight) * slope
        grad_pre_low = grad_pre.astype(BF16)
        d_fc_bias = jnp.sum(grad_pre, axis=(0, 1))
        fc_half = wgrad_cols(normed_two, grad_pre_low, pos, 1280)
        proj_state = cross_first(proj_kept, pos)
        fc_sent = flip(fc_half, CORE_BIT)
        grad_norm = einsum("bsf,wf->bsw", after(grad_pre_low, fc_half, *proj_state[:2]), fc_weight)
        fc_kept = wgrad_cols(normed_two, grad_pre_low, pos, 1280, fc_sent)
        grad_ln, d_ln2_gain, d_ln2_bias = layer_norm_bwd(grad_norm, hat_two, inv_two, ln2_gain)
        grad_middle = grad_wide + grad_ln
        grad_middle_low = after(grad_middle.astype(BF16), fc_kept[2], fc_kept[3])
        d_out_bias = jnp.sum(grad_middle, axis=(0, 1))
        out_half = wgrad_cols(mixed, grad_middle_low, pos, 640)
        out_sent = flip(out_half, CORE_BIT)
        grad_mixed = einsum("bsv,wv->bsw", after(grad_middle_low, out_half), out_weight).astype(BF16)
        out_kept = wgrad_cols(mixed, grad_middle_low, pos, 640, out_sent)
        grad_qkv, qkv_sums = attn_bwd(qkv, after(grad_mixed, out_kept[2], out_kept[3]), lse)
        fc_state = cross_first(held(fc_kept, qkv_sums), pos)
        qkv_half = wgrad_cols(normed_one, after(grad_qkv, *fc_state[:2]), pos, 1920)
        out_state = cross_first(held(out_kept, qkv_half), pos)
        qkv_sent = flip(qkv_half, CORE_BIT)
        d_qkv_bias = jnp.sum(qkv_sums, axis=(0, 1))
        grad_norm = einsum("bsk,wk->bsw", after(grad_qkv, qkv_half, *out_state[:2]), qkv_weight)
        grad_ln, d_ln1_gain, d_ln1_bias = layer_norm_bwd(grad_norm, hat_one, inv_one, ln1_gain)
        grad_in = (grad_middle + grad_ln).astype(BF16)
        small = (d_ln1_gain, d_ln1_bias, d_qkv_bias, d_out_bias, d_ln2_gain, d_ln2_bias, d_fc_bias, d_proj_bias)
        rows = jnp.concatenate([s.reshape(n, -1) for s in small], axis=1)
        rows = jnp.pad(rows, ((0, 0), (0, 3072 - rows.shape[1])))
        summed = sum_scatter(rows.reshape(n, 24, 128)).reshape(-1)
        qkv_kept = wgrad_cols(normed_one, after(grad_qkv, summed), pos, 1920, qkv_sent)
        tail_hidden = after(hidden, qkv_kept[2], qkv_kept[3])
        resid_out = (middle_wide + einsum("bsf,fw->bsw", tail_hidden, proj_weight) + proj_bias).astype(BF16)
        qkv_state = cross_first(held(qkv_kept, resid_out), pos)
        d_proj_weight = jnp.concatenate(cross_second(proj_state, pos), axis=1)
        d_fc_weight = finish_cols(*cross_second(fc_state, pos), pos)
        d_out_weight = finish_cols(*cross_second(out_state, pos), pos)
        d_qkv_weight = finish_cols(*cross_second(qkv_state, pos), pos)

        shards, at = [], 0
        for vec in small:
            shards.append(summed[at:at + vec.shape[0] // n])
            at += vec.shape[0] // n
        (d_ln1_gain, d_ln1_bias, d_qkv_bias, d_out_bias, d_ln2_gain, d_ln2_bias, d_fc_bias, d_proj_bias) = shards
        return (resid_out, grad_in, d_ln1_gain, d_ln1_bias, d_qkv_weight, d_qkv_bias, d_out_weight, d_out_bias,
                d_ln2_gain, d_ln2_bias, d_fc_weight, d_fc_bias, d_proj_weight, d_proj_bias)

    return jax.shard_map(device_step, mesh=mesh, in_specs=specs, out_specs=specs, check_vma=False)
```

```python
import functools
import math

import jax
import jax.numpy as jnp
from jax import lax
from jax.experimental import pallas as pl
from jax.experimental.pallas import tpu as pltpu
from jax.sharding import PartitionSpec as P

HEADS = 16
WIDTH = 1280
HEAD_DIM = 80
GROUP = 8
GROUP_COLS = GROUP * HEAD_DIM
ROWS = 640
CORE_BIT, X_BIT, Y_BIT = 1, 2, 4
SCALE = HEAD_DIM ** -0.5
LOG2E = math.log2(math.e)
LN_EPS = 1e-5
F32 = jnp.float32
BF16 = jnp.bfloat16
VMEM_LIMIT = 60 * 2 ** 20


def dot(lhs, rhs, lhs_dim, rhs_dim):
    return lax.dot_general(lhs, rhs, (((lhs_dim,), (rhs_dim,)), ((), ())), preferred_element_type=F32)


def attn_fwd_kernel(q_ref, k_ref, v_ref, o_ref, lse_ref):
    for head in range(GROUP):
        cols = slice(head * HEAD_DIM, (head + 1) * HEAD_DIM)
        scores = dot(k_ref[0, :, cols], q_ref[0, :, cols], 1, 1)
        top = jnp.max(scores, axis=0, keepdims=True)
        expo = jnp.exp2((scores - top) * (SCALE * LOG2E))
        total = jnp.sum(expo, axis=0, keepdims=True)
        probs = (expo * (1.0 / total)).astype(BF16)
        o_ref[0, :, cols] = dot(probs, v_ref[0, :, cols], 0, 0).astype(BF16)
        lse_ref[0, 0, head:head + 1, :] = top * (SCALE * LOG2E) + jnp.log2(total)


def attn_bwd_kernel(q_ref, k_ref, v_ref, do_ref, lse_ref, dqkv_ref, dbias_ref, dq_ref, dk_ref, dv_ref, sums_ref):
    for head in range(GROUP):
        cols = slice(head * HEAD_DIM, (head + 1) * HEAD_DIM)
        q, k, v, do = q_ref[0, :, cols], k_ref[0, :, cols], v_ref[0, :, cols], do_ref[0, :, cols]
        scores = dot(k, q, 1, 1)
        probs = jnp.exp2(scores * (SCALE * LOG2E) - lse_ref[0, 0, head:head + 1, :])
        grad_probs = dot(v, do, 1, 1)
        grad_v = dot(probs.astype(BF16), do, 1, 0)
        delta = jnp.sum(probs * grad_probs, axis=0, keepdims=True)
        grad_scores = (probs * ((grad_probs - delta) * SCALE)).astype(BF16)
        grad_k = dot(grad_scores, q, 1, 0)
        grad_q = dot(grad_scores, k, 0, 0)
        for part, (grad, ref) in enumerate(((grad_q, dq_ref), (grad_k, dk_ref), (grad_v, dv_ref))):
            ref[:, cols] = grad.astype(BF16)
            sums_ref[part, :, cols] = jnp.sum(grad, axis=0, keepdims=True)
    width = dqkv_ref.shape[2] // 3
    for part, ref in enumerate((dq_ref, dk_ref, dv_ref)):
        cols = pl.ds(pl.multiple_of(part * width + pl.program_id(1) * GROUP_COLS, 128), GROUP_COLS)
        dqkv_ref[0, :, cols] = ref[...]
        dbias_ref[0, :, cols] = sums_ref[part]


def attn_specs(qkv):
    images, seq_len, _ = qkv.shape
    groups = qkv.shape[2] // 3 // GROUP_COLS

    def cols(part):
        return pl.BlockSpec((1, seq_len, GROUP_COLS), lambda b, g: (b, 0, part * groups + g))

    lse = pl.BlockSpec((1, 1, GROUP, seq_len), lambda b, g: (b, g, 0, 0))
    return images, seq_len, groups, cols, lse


def attn_fwd(qkv):
    images, seq_len, groups, cols, lse = attn_specs(qkv)
    width = groups * GROUP_COLS
    return pl.pallas_call(
        attn_fwd_kernel, grid=(images, groups), name="attn_fwd",
        in_specs=[cols(0), cols(1), cols(2)], out_specs=[cols(0), lse],
        out_shape=[jax.ShapeDtypeStruct((images, seq_len, width), BF16),
                   jax.ShapeDtypeStruct((images, groups, GROUP, seq_len), F32)],
        cost_estimate=pl.CostEstimate(flops=30 * 10 ** 9, bytes_accessed=16 * 10 ** 6, transcendentals=0),
        compiler_params=pltpu.CompilerParams(vmem_limit_bytes=VMEM_LIMIT))(qkv, qkv, qkv)


def attn_bwd(qkv, grad_mixed, lse_vals):
    images, seq_len, groups, cols, lse = attn_specs(qkv)
    out_cols = qkv.shape[2]
    return pl.pallas_call(
        attn_bwd_kernel, grid=(images, groups), name="attn_bwd",
        in_specs=[cols(0), cols(1), cols(2), cols(0), lse],
        out_specs=[pl.BlockSpec((1, seq_len, out_cols), lambda b, g: (b, 0, 0)),
                   pl.BlockSpec((1, 1, out_cols), lambda b, g: (b, 0, 0))],
        out_shape=[jax.ShapeDtypeStruct((images, seq_len, out_cols), BF16),
                   jax.ShapeDtypeStruct((images, 1, out_cols), F32)],
        scratch_shapes=[pltpu.VMEM((seq_len, GROUP_COLS), BF16)] * 3 + [pltpu.VMEM((3, 1, GROUP_COLS), F32)],
        cost_estimate=pl.CostEstimate(flops=50 * 10 ** 9, bytes_accessed=30 * 10 ** 6, transcendentals=0),
        compiler_params=pltpu.CompilerParams(vmem_limit_bytes=VMEM_LIMIT))(qkv, qkv, qkv, grad_mixed, lse_vals)


def fc_gelu_kernel(x_ref, w_ref, b_ref, h_ref, slope_ref):
    for image in range(x_ref.shape[0]):
        pre = dot(x_ref[image], w_ref[...], 1, 0) + b_ref[...]
        cdf = 0.5 + 0.5 * lax.erf(pre * (0.5 ** 0.5))
        pdf = jnp.exp2(pre * pre * (-0.5 * LOG2E)) * ((2.0 * math.pi) ** -0.5)
        h_ref[image] = (pre * cdf).astype(BF16)
        slope_ref[image] = cdf + pre * pdf


def fc_gelu(normed, weight, bias, tile=512):
    images, seq_len, width = normed.shape
    ffn = weight.shape[1]
    out = pl.BlockSpec((images, seq_len, tile), lambda j: (0, 0, j))
    return pl.pallas_call(
        fc_gelu_kernel, grid=(ffn // tile,), name="fc_gelu",
        in_specs=[pl.BlockSpec((images, seq_len, width), lambda j: (0, 0, 0)),
                  pl.BlockSpec((width, tile), lambda j: (0, j)), pl.BlockSpec((1, tile), lambda j: (0, j))],
        out_specs=[out, out],
        out_shape=[jax.ShapeDtypeStruct((images, seq_len, ffn), BF16),
                   jax.ShapeDtypeStruct((images, seq_len, ffn), F32)],
        cost_estimate=pl.CostEstimate(flops=30 * 10 ** 9, bytes_accessed=60 * 10 ** 6, transcendentals=0),
        compiler_params=pltpu.CompilerParams(vmem_limit_bytes=VMEM_LIMIT))(normed, weight, bias.reshape(1, ffn))


def wgrad_kernel(acts_ref, grad_ref, keep_a, keep_b, send_a, send_b, total, sent, recv, send_sem, recv_sem, *,
                 piece, by_rows):
    me = lax.axis_index("fsdp")
    y, x, partner = me // Y_BIT, (me // X_BIT) % 2, me + 1 - 2 * (me % 2)
    phase, step = pl.program_id(0), pl.program_id(2)
    tile = pl.program_id(1) * pl.num_programs(2) + step
    tiles = sent.shape[0]
    barrier = pltpu.get_barrier_semaphore()

    @pl.when((phase == 0) & (tile == 0))
    def _():
        pl.semaphore_signal(barrier, inc=1, device_id=(partner,), device_id_type=pl.DeviceIdType.MESH)
        pl.semaphore_wait(barrier, 1)

    def swap(index):
        return pltpu.make_async_remote_copy(
            src_ref=sent.at[index], dst_ref=recv.at[index], send_sem=send_sem.at[index], recv_sem=recv_sem.at[index],
            device_id=(partner,), device_id_type=pl.DeviceIdType.MESH)

    @pl.when((phase == 0) & (tile > 0))
    def _():
        swap(tile - 1).start()

    @pl.when((phase == 1) & (tile == 0))
    def _():
        swap(tiles - 1).start()

    product = dot(acts_ref[0], grad_ref[0], 0, 0)
    for image in range(1, acts_ref.shape[0]):
        product += dot(acts_ref[image], grad_ref[image], 0, 0)

    @pl.when(phase == 0)
    def _():
        sent[tile] = product.astype(BF16)

    def put(to_a, row_y, row_x, rows, cols):
        mine = row_x == x if to_a else row_y == y
        keep, send, slot = (keep_a, send_a, row_y) if to_a else (keep_b, send_b, row_x)

        @pl.when(mine)
        def _():
            keep[slot] = total[rows, cols]

        @pl.when(jnp.logical_not(mine))
        def _():
            send[slot] = total[rows, cols].astype(BF16)

    @pl.when(phase == 1)
    def _():
        swap(tile).wait_recv()
        total[...] = product + recv[tile].astype(F32)
        if by_rows:
            half = total.shape[1] // 2
            put(True, step // 2, step % 2, slice(None), slice(0, half))
            put(False, step // 2, step % 2, slice(None), slice(half, 2 * half))
        else:
            for block in range(ROWS // piece):
                put(block % 2 == 0, step, block // 2, slice(block * piece, (block + 1) * piece), slice(None))

    @pl.when((phase == 1) & (tile == tiles - 1))
    def _():
        for index in range(tiles):
            swap(index).wait_send()


def wgrad(acts, grad, tile_n, by_rows, ident):
    images, seq_len, depth = acts.shape
    width = grad.shape[2] if by_rows else grad.shape[2] // 2
    blocks, steps, piece = width // tile_n, (4 if by_rows else depth // ROWS), depth // 8
    tiles = blocks * steps

    def half(p):
        return (lax.axis_index("fsdp") + 1 + p) % 2

    if by_rows:
        acts_map, grad_map = (lambda p, j, i: (0, 0, 2 * i + half(p))), (lambda p, j, i: (0, 0, 0))
        kept_block, kept_map, kept_shape = (2, piece, width // 2), (lambda p, j, i: (0, 0, 0)), (2, piece, width // 2)
    else:
        acts_map, grad_map = (lambda p, j, i: (0, 0, i)), (lambda p, j, i: (0, 0, half(p) * blocks + j))
        kept_block, kept_map, kept_shape = (2, piece, tile_n), (lambda p, j, i: (0, 0, p * j)), (2, piece, width)
    return pl.pallas_call(
        functools.partial(wgrad_kernel, piece=piece, by_rows=by_rows), name="wgrad", grid=(2, blocks, steps),
        in_specs=[pl.BlockSpec((images, seq_len, ROWS), acts_map), pl.BlockSpec((images, seq_len, tile_n), grad_map)],
        out_specs=[pl.BlockSpec(kept_block, kept_map)] * 4,
        out_shape=[jax.ShapeDtypeStruct(kept_shape, kind) for kind in (F32, F32, BF16, BF16)],
        scratch_shapes=[pltpu.VMEM((ROWS, tile_n), F32), pltpu.VMEM((tiles, ROWS, tile_n), BF16),
                        pltpu.VMEM((tiles, ROWS, tile_n), BF16), pltpu.SemaphoreType.DMA((tiles,)),
                        pltpu.SemaphoreType.DMA((tiles,))],
        cost_estimate=pl.CostEstimate(flops=2 * images * seq_len * depth * grad.shape[2], bytes_accessed=4 * 10 ** 7,
                                      transcendentals=0),
        compiler_params=pltpu.CompilerParams(collective_id=ident, has_side_effects=True,
                                             vmem_limit_bytes=VMEM_LIMIT))(acts, grad)


OWN_X0, OWN_X1, OWN_Y0, OWN_Y1, FORWARD_X, FORWARD_Y = range(6)
PARTNER_OWN, PARTNER_X0, PARTNER_X1, PARTNER_Y0, PARTNER_Y1, PARTNER_D0, PARTNER_D1 = range(6, 13)
COPIES = 13


def gather_kernel(count, *refs):
    ins, outs, (send_sem, recv_sem, local_sem) = refs[:count], refs[count:2 * count], refs[2 * count:]
    me = lax.axis_index("fsdp")
    x_peer = me + X_BIT - 2 * X_BIT * ((me // X_BIT) % 2)
    y_peer = me + Y_BIT - 2 * Y_BIT * (me // Y_BIT)
    partner = me + 1 - 2 * (me % 2)
    diagonal = x_peer + y_peer - me
    barrier = pltpu.get_barrier_semaphore()
    for peer in (x_peer, y_peer, partner):
        pl.semaphore_signal(barrier, inc=1, device_id=(peer,), device_id_type=pl.DeviceIdType.MESH)
    pl.semaphore_wait(barrier, 3)

    def remote(array, which):
        shard, out = ins[array], outs[array]
        source, slot, peer = {
            OWN_X0: (shard.at[0], 2 * me, x_peer), OWN_X1: (shard.at[1], 2 * me + 1, x_peer),
            OWN_Y0: (shard.at[0], 2 * me, y_peer), OWN_Y1: (shard.at[1], 2 * me + 1, y_peer),
            FORWARD_X: (None, 2 * y_peer + 1, x_peer), FORWARD_Y: (None, 2 * x_peer, y_peer),
            PARTNER_OWN: (shard, None, partner),
            PARTNER_X0: (None, 2 * x_peer, partner), PARTNER_X1: (None, 2 * x_peer + 1, partner),
            PARTNER_Y0: (None, 2 * y_peer, partner), PARTNER_Y1: (None, 2 * y_peer + 1, partner),
            PARTNER_D0: (None, 2 * diagonal, partner), PARTNER_D1: (None, 2 * diagonal + 1, partner)}[which]
        target = out.at[pl.ds(2 * me, 2)] if slot is None else out.at[slot]
        return pltpu.make_async_remote_copy(
            src_ref=target if source is None else source, dst_ref=target,
            send_sem=send_sem.at[array, which], recv_sem=recv_sem.at[array, which],
            device_id=(peer,), device_id_type=pl.DeviceIdType.MESH)

    def local(array):
        return pltpu.make_async_copy(ins[array], outs[array].at[pl.ds(2 * me, 2)], local_sem.at[array])

    def send_own(array):
        for which in (OWN_X0, OWN_Y1, PARTNER_OWN, OWN_X1, OWN_Y0):
            remote(array, which).start()
        local(array).start()

    def on_arrival(array, arrived, *then):
        remote(array, arrived).wait_recv()
        for which in then:
            remote(array, which).start()

    def first_halves(array):
        on_arrival(array, OWN_X0, FORWARD_Y, PARTNER_X0)
        on_arrival(array, OWN_Y1, FORWARD_X, PARTNER_Y1)

    def second_halves(array):
        on_arrival(array, OWN_X1, PARTNER_X1)
        on_arrival(array, OWN_Y0, PARTNER_Y0)

    def diagonals(array):
        on_arrival(array, FORWARD_X, PARTNER_D1)
        on_arrival(array, FORWARD_Y, PARTNER_D0)

    send_own(0)
    for array in range(count):
        first_halves(array)
        if array + 1 < count:
            send_own(array + 1)
        second_halves(array)
        if array > 0:
            diagonals(array - 1)
    diagonals(count - 1)
    for array in range(count):
        for which in range(PARTNER_OWN, COPIES):
            remote(array, which).wait_recv()
        for which in range(COPIES):
            remote(array, which).wait_send()
        local(array).wait()


def gather_now(*shards):
    count = len(shards)
    halves = [s.reshape(2, s.shape[0] // 2, s.shape[1]) for s in shards]
    outs = pl.pallas_call(
        functools.partial(gather_kernel, count), name="gather_now",
        in_specs=[pl.BlockSpec(memory_space=pltpu.VMEM)] * count,
        out_specs=[pl.BlockSpec(memory_space=pltpu.HBM)] * count,
        out_shape=[jax.ShapeDtypeStruct((16,) + h.shape[1:], BF16) for h in halves],
        scratch_shapes=[pltpu.SemaphoreType.DMA((count, COPIES)), pltpu.SemaphoreType.DMA((count, COPIES)),
                        pltpu.SemaphoreType.DMA((count,))],
        cost_estimate=pl.CostEstimate(flops=50 * 10 ** 9, bytes_accessed=10 ** 7, transcendentals=0),
        compiler_params=pltpu.CompilerParams(collective_id=1, has_side_effects=True))(*halves)
    return [o.reshape(8 * s.shape[0], s.shape[1]) for o, s in zip(outs, shards)]


def layer_norm_fwd(values, gain, bias):
    mean_val = jnp.mean(values, axis=-1, keepdims=True)
    centered = values - mean_val
    inv_std = lax.rsqrt(jnp.mean(centered * centered, axis=-1, keepdims=True) + LN_EPS)
    x_hat = centered * inv_std
    return x_hat * gain + bias, x_hat, inv_std


def layer_norm_bwd(grad_norm, x_hat, inv_std, gain):
    grad_hat = grad_norm * gain
    grad_vals = inv_std * (grad_hat - jnp.mean(grad_hat, axis=-1, keepdims=True)
                           - x_hat * jnp.mean(grad_hat * x_hat, axis=-1, keepdims=True))
    return grad_vals, jnp.sum(grad_norm * x_hat, axis=(0, 1)), jnp.sum(grad_norm, axis=(0, 1))


def einsum(spec, lhs, rhs):
    return jnp.einsum(spec, lhs, rhs, preferred_element_type=F32)


def flip(value, bit):
    return lax.ppermute(value, "fsdp", [(d, d ^ bit) for d in range(8)])


def pick(value, index):
    return lax.dynamic_index_in_dim(value, index, 0, keepdims=False).astype(F32)


def after(value, *done):
    return lax.optimization_barrier((value,) + done)[0]


def held(kept, *done):
    keep_a, keep_b = lax.optimization_barrier((kept[0], kept[1]) + done)[:2]
    return keep_a, keep_b, kept[2], kept[3]


def cross_first(name, kept, pos):
    keep_a, keep_b, send_a, send_b = kept
    y, x = pos[0], pos[1]
    with jax.named_scope(name + "_cross_one"):
        recv_a, recv_b = flip(send_a, X_BIT), flip(send_b, Y_BIT)
    next_a = (pick(keep_a, 1 - y) + pick(recv_a, 1 - y)).astype(BF16)
    next_b = (pick(keep_b, 1 - x) + pick(recv_b, 1 - x)).astype(BF16)
    return next_a, next_b, keep_a, keep_b, recv_a, recv_b


def cross_second(name, state, pos):
    next_a, next_b, keep_a, keep_b, recv_a, recv_b = state
    y, x = pos[0], pos[1]
    with jax.named_scope(name + "_cross_two"):
        last_a, last_b = flip(next_a, Y_BIT), flip(next_b, X_BIT)
    return (pick(keep_a, y) + pick(recv_a, y) + last_a.astype(F32),
            pick(keep_b, x) + pick(recv_b, x) + last_b.astype(F32))


def finish_cols(sum_a, sum_b, pos):
    core = pos[2]
    mine = jnp.where(core == 0, sum_a, sum_b)
    other = flip(jnp.where(core == 0, sum_b, sum_a), CORE_BIT)
    return jnp.where(core == 0, jnp.concatenate([mine, other], axis=1), jnp.concatenate([other, mine], axis=1))


def sum_kernel(n, in_ref, out_ref, recv, send_sem, recv_sem):
    me = lax.axis_index("fsdp")
    barrier = pltpu.get_barrier_semaphore()
    peers = [lax.rem(me + step, n) for step in range(1, n)]
    for peer in peers:
        pl.semaphore_signal(barrier, inc=1, device_id=(peer,), device_id_type=pl.DeviceIdType.MESH)
    pl.semaphore_wait(barrier, n - 1)
    copies = []
    for step, peer in enumerate(peers):
        copies.append(pltpu.make_async_remote_copy(
            src_ref=in_ref.at[peer], dst_ref=recv.at[step], send_sem=send_sem.at[step], recv_sem=recv_sem.at[step],
            device_id=(peer,), device_id_type=pl.DeviceIdType.MESH))
        copies[-1].start()
    total = in_ref[me]
    for step, copy in enumerate(copies):
        copy.wait()
        total += recv[step]
    out_ref[...] = total


def sum_scatter(values):
    n, rows, cols = values.shape
    return pl.pallas_call(
        functools.partial(sum_kernel, n), name="sum_scatter",
        in_specs=[pl.BlockSpec(memory_space=pltpu.VMEM)], out_specs=pl.BlockSpec(memory_space=pltpu.VMEM),
        out_shape=jax.ShapeDtypeStruct((rows, cols), F32),
        scratch_shapes=[pltpu.VMEM((n - 1, rows, cols), F32), pltpu.SemaphoreType.DMA((n - 1,)),
                        pltpu.SemaphoreType.DMA((n - 1,))],
        cost_estimate=pl.CostEstimate(flops=4 * 10 ** 9, bytes_accessed=10 ** 6, transcendentals=0),
        compiler_params=pltpu.CompilerParams(collective_id=0, has_side_effects=True))(values)


def solution(mesh):
    specs = (P("fsdp"),) * 14
    n = mesh.shape["fsdp"]

    def gather(shard):
        return lax.all_gather(shard.astype(BF16), "fsdp", axis=0, tiled=True)

    def device_step(resid_in, grad_out, ln1_gain, ln1_bias, qkv_weight, qkv_bias, out_weight, out_bias,
                    ln2_gain, ln2_bias, fc_weight, fc_bias, proj_weight, proj_bias):
        vectors = (ln1_gain, ln1_bias, qkv_bias, out_bias, ln2_gain, ln2_bias, fc_bias, proj_bias)
        lane_rows = [jnp.pad(v, (0, -v.shape[0] % 128)).reshape(-1, 128) for v in vectors]
        packed = jnp.concatenate(lane_rows).astype(BF16)
        packed = lax.optimization_barrier(jnp.pad(packed, ((0, 32 - packed.shape[0]), (0, 0))))
        packed, qkv_weight, out_weight = gather_now(packed, qkv_weight.astype(BF16), out_weight.astype(BF16))
        fc_weight, proj_weight = [gather(after(w, packed)) for w in (fc_weight, proj_weight)]
        packed = lax.optimization_barrier(packed).astype(F32).reshape(n, 32, 128)
        full, at = [], 0
        for vec in vectors:
            count = -(-vec.shape[0] // 128)
            full.append(packed[:, at:at + count].reshape(n, count * 128)[:, :vec.shape[0]].reshape(-1))
            at += count
        ln1_gain, ln1_bias, qkv_bias, out_bias, ln2_gain, ln2_bias, fc_bias, proj_bias = [f.astype(F32) for f in full]

        resid = resid_in.astype(F32)
        normed, hat_one, inv_one = layer_norm_fwd(resid, ln1_gain, ln1_bias)
        normed_one = normed.astype(BF16)
        qkv = (einsum("bsw,wk->bsk", normed_one, qkv_weight) + qkv_bias).astype(BF16)
        mixed, lse = attn_fwd(qkv)
        middle = (resid + einsum("bsw,wv->bsv", mixed, out_weight) + out_bias).astype(BF16)
        middle_wide = middle.astype(F32)
        normed, hat_two, inv_two = layer_norm_fwd(middle_wide, ln2_gain, ln2_bias)
        normed_two = normed.astype(BF16)
        hidden, slope = fc_gelu(normed_two, fc_weight, fc_bias)

        device = lax.axis_index("fsdp")
        pos = jnp.stack([device // Y_BIT, (device // X_BIT) % 2, device % 2]).astype(jnp.int32)
        grad_wide = grad_out.astype(F32)
        d_proj_bias = jnp.sum(grad_wide, axis=(0, 1))
        proj_kept = wgrad(hidden, grad_out, WIDTH, True, 2)
        with jax.named_scope("dgrad_hidden"):
            grad_pre = einsum("bsw,fw->bsf", after(grad_out, *proj_kept[2:]), proj_weight) * slope
            grad_pre_low = grad_pre.astype(BF16)
        d_fc_bias = jnp.sum(grad_pre, axis=(0, 1))
        fc_kept = wgrad(normed_two, grad_pre_low, 1280, False, 3)
        proj_state = cross_first("proj", held(proj_kept, fc_kept[2]), pos)
        with jax.named_scope("dgrad_fc"):
            grad_norm = einsum("bsf,wf->bsw", after(grad_pre_low, *fc_kept[2:], *proj_state[:2]), fc_weight)
        grad_ln, d_ln2_gain, d_ln2_bias = layer_norm_bwd(grad_norm, hat_two, inv_two, ln2_gain)
        grad_middle = grad_wide + grad_ln
        grad_middle_low = grad_middle.astype(BF16)
        d_out_bias = jnp.sum(grad_middle, axis=(0, 1))
        out_kept = wgrad(mixed, grad_middle_low, 640, False, 4)
        with jax.named_scope("dgrad_out"):
            grad_mixed = einsum("bsv,wv->bsw", after(grad_middle_low, *out_kept[2:]), out_weight).astype(BF16)
        with jax.named_scope("attn_bwd_call"):
            grad_qkv, qkv_sums = attn_bwd(qkv, grad_mixed, lse)
        fc_state = cross_first("fc", held(fc_kept, qkv_sums), pos)
        out_state = cross_first("out", held(out_kept, qkv_sums), pos)
        d_qkv_bias = jnp.sum(qkv_sums, axis=(0, 1))
        with jax.named_scope("dgrad_qkv"):
            grad_norm = einsum("bsk,wk->bsw", after(grad_qkv, *fc_state[:2], *out_state[:2]), qkv_weight)
        grad_ln, d_ln1_gain, d_ln1_bias = layer_norm_bwd(grad_norm, hat_one, inv_one, ln1_gain)
        grad_in = (grad_middle + grad_ln).astype(BF16)
        small = (d_ln1_gain, d_ln1_bias, d_qkv_bias, d_out_bias, d_ln2_gain, d_ln2_bias, d_fc_bias, d_proj_bias)
        rows = jnp.concatenate([s.reshape(n, -1) for s in small], axis=1)
        rows = jnp.pad(rows, ((0, 0), (0, 3072 - rows.shape[1])))
        summed = sum_scatter(rows.reshape(n, 24, 128)).reshape(-1)
        qkv_kept = wgrad(normed_one, after(grad_qkv, summed), 1920, False, 5)
        tail_hidden = after(hidden, *qkv_kept[2:])
        with jax.named_scope("resid_product"):
            product = einsum("bsf,fw->bsw", tail_hidden, proj_weight)
        resid_out = (middle_wide + product + proj_bias).astype(BF16)
        qkv_state = cross_first("qkv", held(qkv_kept, resid_out), pos)
        d_proj_weight = jnp.concatenate(cross_second("proj", proj_state, pos), axis=1)
        d_fc_weight = finish_cols(*cross_second("fc", fc_state, pos), pos)
        d_out_weight = finish_cols(*cross_second("out", out_state, pos), pos)
        d_qkv_weight = finish_cols(*cross_second("qkv", qkv_state, pos), pos)

        shards, at = [], 0
        for vec in small:
            shards.append(summed[at:at + vec.shape[0] // n])
            at += vec.shape[0] // n
        (d_ln1_gain, d_ln1_bias, d_qkv_bias, d_out_bias, d_ln2_gain, d_ln2_bias, d_fc_bias, d_proj_bias) = shards
        return (resid_out, grad_in, d_ln1_gain, d_ln1_bias, d_qkv_weight, d_qkv_bias, d_out_weight, d_out_bias,
                d_ln2_gain, d_ln2_bias, d_fc_weight, d_fc_bias, d_proj_weight, d_proj_bias)

    return jax.shard_map(device_step, mesh=mesh, in_specs=specs, out_specs=specs, check_vma=False)
```

```python
import functools
import math

import jax
import jax.numpy as jnp
from jax import lax
from jax.experimental import pallas as pl
from jax.experimental.pallas import tpu as pltpu
from jax.sharding import PartitionSpec as P

HEADS = 16
WIDTH = 1280
HEAD_DIM = 80
GROUP = 8
GROUP_COLS = GROUP * HEAD_DIM
ROWS = 640
CORE_BIT, X_BIT, Y_BIT = 1, 2, 4
SCALE = HEAD_DIM ** -0.5
LOG2E = math.log2(math.e)
LN_EPS = 1e-5
F32 = jnp.float32
BF16 = jnp.bfloat16
VMEM_LIMIT = 60 * 2 ** 20


def dot(lhs, rhs, lhs_dim, rhs_dim):
    return lax.dot_general(lhs, rhs, (((lhs_dim,), (rhs_dim,)), ((), ())), preferred_element_type=F32)


def attn_fwd_kernel(q_ref, k_ref, v_ref, o_ref, lse_ref):
    for head in range(GROUP):
        cols = slice(head * HEAD_DIM, (head + 1) * HEAD_DIM)
        scores = dot(k_ref[0, :, cols], q_ref[0, :, cols], 1, 1)
        top = jnp.max(scores, axis=0, keepdims=True)
        expo = jnp.exp2((scores - top) * (SCALE * LOG2E))
        total = jnp.sum(expo, axis=0, keepdims=True)
        probs = (expo * (1.0 / total)).astype(BF16)
        o_ref[0, :, cols] = dot(probs, v_ref[0, :, cols], 0, 0).astype(BF16)
        lse_ref[0, 0, head:head + 1, :] = top * (SCALE * LOG2E) + jnp.log2(total)


def attn_bwd_kernel(q_ref, k_ref, v_ref, do_ref, lse_ref, dqkv_ref, dbias_ref, dq_ref, dk_ref, dv_ref, sums_ref):
    for head in range(GROUP):
        cols = slice(head * HEAD_DIM, (head + 1) * HEAD_DIM)
        q, k, v, do = q_ref[0, :, cols], k_ref[0, :, cols], v_ref[0, :, cols], do_ref[0, :, cols]
        scores = dot(k, q, 1, 1)
        probs = jnp.exp2(scores * (SCALE * LOG2E) - lse_ref[0, 0, head:head + 1, :])
        grad_probs = dot(v, do, 1, 1)
        grad_v = dot(probs.astype(BF16), do, 1, 0)
        delta = jnp.sum(probs * grad_probs, axis=0, keepdims=True)
        grad_scores = (probs * (grad_probs - delta)).astype(BF16)
        grad_k = dot(grad_scores, q, 1, 0) * SCALE
        grad_q = dot(grad_scores, k, 0, 0) * SCALE
        for part, (grad, ref) in enumerate(((grad_q, dq_ref), (grad_k, dk_ref), (grad_v, dv_ref))):
            ref[:, cols] = grad.astype(BF16)
            sums_ref[part, :, cols] = jnp.sum(grad, axis=0, keepdims=True)
    width = dqkv_ref.shape[2] // 3
    for part, ref in enumerate((dq_ref, dk_ref, dv_ref)):
        cols = pl.ds(pl.multiple_of(part * width + pl.program_id(1) * GROUP_COLS, 128), GROUP_COLS)
        dqkv_ref[0, :, cols] = ref[...]
        dbias_ref[0, :, cols] = sums_ref[part]


def attn_specs(qkv):
    images, seq_len, _ = qkv.shape
    groups = qkv.shape[2] // 3 // GROUP_COLS

    def cols(part):
        return pl.BlockSpec((1, seq_len, GROUP_COLS), lambda b, g: (b, 0, part * groups + g))

    lse = pl.BlockSpec((1, 1, GROUP, seq_len), lambda b, g: (b, g, 0, 0))
    return images, seq_len, groups, cols, lse


def attn_fwd(qkv):
    images, seq_len, groups, cols, lse = attn_specs(qkv)
    width = groups * GROUP_COLS
    return pl.pallas_call(
        attn_fwd_kernel, grid=(images, groups), name="attn_fwd",
        in_specs=[cols(0), cols(1), cols(2)], out_specs=[cols(0), lse],
        out_shape=[jax.ShapeDtypeStruct((images, seq_len, width), BF16),
                   jax.ShapeDtypeStruct((images, groups, GROUP, seq_len), F32)],
        cost_estimate=pl.CostEstimate(flops=30 * 10 ** 9, bytes_accessed=16 * 10 ** 6, transcendentals=0),
        compiler_params=pltpu.CompilerParams(vmem_limit_bytes=VMEM_LIMIT))(qkv, qkv, qkv)


def attn_bwd(qkv, grad_mixed, lse_vals):
    images, seq_len, groups, cols, lse = attn_specs(qkv)
    out_cols = qkv.shape[2]
    return pl.pallas_call(
        attn_bwd_kernel, grid=(images, groups), name="attn_bwd",
        in_specs=[cols(0), cols(1), cols(2), cols(0), lse],
        out_specs=[pl.BlockSpec((1, seq_len, out_cols), lambda b, g: (b, 0, 0)),
                   pl.BlockSpec((1, 1, out_cols), lambda b, g: (b, 0, 0))],
        out_shape=[jax.ShapeDtypeStruct((images, seq_len, out_cols), BF16),
                   jax.ShapeDtypeStruct((images, 1, out_cols), F32)],
        scratch_shapes=[pltpu.VMEM((seq_len, GROUP_COLS), BF16)] * 3 + [pltpu.VMEM((3, 1, GROUP_COLS), F32)],
        cost_estimate=pl.CostEstimate(flops=50 * 10 ** 9, bytes_accessed=30 * 10 ** 6, transcendentals=0),
        compiler_params=pltpu.CompilerParams(vmem_limit_bytes=VMEM_LIMIT))(qkv, qkv, qkv, grad_mixed, lse_vals)


def fc_gelu_kernel(x_ref, w_ref, b_ref, h_ref, slope_ref):
    for image in range(x_ref.shape[0]):
        pre = dot(x_ref[image], w_ref[...], 1, 0) + b_ref[...]
        cdf = 0.5 + 0.5 * lax.erf(pre * (0.5 ** 0.5))
        pdf = jnp.exp2(pre * pre * (-0.5 * LOG2E)) * ((2.0 * math.pi) ** -0.5)
        h_ref[image] = (pre * cdf).astype(BF16)
        slope_ref[image] = cdf + pre * pdf


def fc_gelu(normed, weight, bias, tile=512):
    images, seq_len, width = normed.shape
    ffn = weight.shape[1]
    out = pl.BlockSpec((images, seq_len, tile), lambda j: (0, 0, j))
    return pl.pallas_call(
        fc_gelu_kernel, grid=(ffn // tile,), name="fc_gelu",
        in_specs=[pl.BlockSpec((images, seq_len, width), lambda j: (0, 0, 0)),
                  pl.BlockSpec((width, tile), lambda j: (0, j)), pl.BlockSpec((1, tile), lambda j: (0, j))],
        out_specs=[out, out],
        out_shape=[jax.ShapeDtypeStruct((images, seq_len, ffn), BF16),
                   jax.ShapeDtypeStruct((images, seq_len, ffn), F32)],
        cost_estimate=pl.CostEstimate(flops=30 * 10 ** 9, bytes_accessed=60 * 10 ** 6, transcendentals=0),
        compiler_params=pltpu.CompilerParams(vmem_limit_bytes=VMEM_LIMIT))(normed, weight, bias.reshape(1, ffn))


def wgrad_kernel(acts_ref, grad_ref, keep_a, keep_b, send_a, send_b, total, sent, recv, send_sem, recv_sem, *,
                 piece, by_rows):
    me = lax.axis_index("fsdp")
    y, x, partner = me // Y_BIT, (me // X_BIT) % 2, me + 1 - 2 * (me % 2)
    phase, step = pl.program_id(0), pl.program_id(2)
    tile = pl.program_id(1) * pl.num_programs(2) + step
    tiles = sent.shape[0]
    barrier = pltpu.get_barrier_semaphore()

    @pl.when((phase == 0) & (tile == 0))
    def _():
        pl.semaphore_signal(barrier, inc=1, device_id=(partner,), device_id_type=pl.DeviceIdType.MESH)
        pl.semaphore_wait(barrier, 1)

    def swap(index):
        return pltpu.make_async_remote_copy(
            src_ref=sent.at[index], dst_ref=recv.at[index], send_sem=send_sem.at[index], recv_sem=recv_sem.at[index],
            device_id=(partner,), device_id_type=pl.DeviceIdType.MESH)

    @pl.when((phase == 0) & (tile > 0))
    def _():
        swap(tile - 1).start()

    @pl.when((phase == 1) & (tile == 0))
    def _():
        swap(tiles - 1).start()

    product = dot(acts_ref[0], grad_ref[0], 0, 0)
    for image in range(1, acts_ref.shape[0]):
        product += dot(acts_ref[image], grad_ref[image], 0, 0)

    @pl.when(phase == 0)
    def _():
        sent[tile] = product.astype(BF16)

    def put(to_a, row_y, row_x, rows, cols):
        mine = row_x == x if to_a else row_y == y
        keep, send, slot = (keep_a, send_a, row_y) if to_a else (keep_b, send_b, row_x)

        @pl.when(mine)
        def _():
            keep[slot] = total[rows, cols]

        @pl.when(jnp.logical_not(mine))
        def _():
            send[slot] = total[rows, cols].astype(BF16)

    @pl.when(phase == 1)
    def _():
        swap(tile).wait_recv()
        total[...] = product + recv[tile].astype(F32)
        if by_rows:
            half = total.shape[1] // 2
            put(True, step // 2, step % 2, slice(None), slice(0, half))
            put(False, step // 2, step % 2, slice(None), slice(half, 2 * half))
        else:
            for block in range(ROWS // piece):
                put(block % 2 == 0, step, block // 2, slice(block * piece, (block + 1) * piece), slice(None))

    @pl.when((phase == 1) & (tile == tiles - 1))
    def _():
        for index in range(tiles):
            swap(index).wait_send()


def wgrad(acts, grad, tile_n, by_rows, ident):
    images, seq_len, depth = acts.shape
    width = grad.shape[2] if by_rows else grad.shape[2] // 2
    blocks, steps, piece = width // tile_n, (4 if by_rows else depth // ROWS), depth // 8
    tiles = blocks * steps

    def half(p):
        return (lax.axis_index("fsdp") + 1 + p) % 2

    if by_rows:
        acts_map, grad_map = (lambda p, j, i: (0, 0, 2 * i + half(p))), (lambda p, j, i: (0, 0, 0))
        kept_block, kept_map, kept_shape = (2, piece, width // 2), (lambda p, j, i: (0, 0, 0)), (2, piece, width // 2)
    else:
        acts_map, grad_map = (lambda p, j, i: (0, 0, i)), (lambda p, j, i: (0, 0, half(p) * blocks + j))
        kept_block, kept_map, kept_shape = (2, piece, tile_n), (lambda p, j, i: (0, 0, p * j)), (2, piece, width)
    return pl.pallas_call(
        functools.partial(wgrad_kernel, piece=piece, by_rows=by_rows), name="wgrad", grid=(2, blocks, steps),
        in_specs=[pl.BlockSpec((images, seq_len, ROWS), acts_map), pl.BlockSpec((images, seq_len, tile_n), grad_map)],
        out_specs=[pl.BlockSpec(kept_block, kept_map)] * 4,
        out_shape=[jax.ShapeDtypeStruct(kept_shape, kind) for kind in (F32, F32, BF16, BF16)],
        scratch_shapes=[pltpu.VMEM((ROWS, tile_n), F32), pltpu.VMEM((tiles, ROWS, tile_n), BF16),
                        pltpu.VMEM((tiles, ROWS, tile_n), BF16), pltpu.SemaphoreType.DMA((tiles,)),
                        pltpu.SemaphoreType.DMA((tiles,))],
        cost_estimate=pl.CostEstimate(flops=2 * images * seq_len * depth * grad.shape[2], bytes_accessed=4 * 10 ** 7,
                                      transcendentals=0),
        compiler_params=pltpu.CompilerParams(collective_id=ident, has_side_effects=True,
                                             vmem_limit_bytes=VMEM_LIMIT))(acts, grad)


OWN_X0, OWN_X1, OWN_Y0, OWN_Y1, FORWARD_X, FORWARD_Y = range(6)
PARTNER_OWN, PARTNER_X0, PARTNER_X1, PARTNER_Y0, PARTNER_Y1, PARTNER_D0, PARTNER_D1 = range(6, 13)
COPIES = 13


def gather_kernel(count, *refs):
    ins, outs, (send_sem, recv_sem, local_sem) = refs[:count], refs[count:2 * count], refs[2 * count:]
    me = lax.axis_index("fsdp")
    x_peer = me + X_BIT - 2 * X_BIT * ((me // X_BIT) % 2)
    y_peer = me + Y_BIT - 2 * Y_BIT * (me // Y_BIT)
    partner = me + 1 - 2 * (me % 2)
    diagonal = x_peer + y_peer - me
    barrier = pltpu.get_barrier_semaphore()
    for peer in (x_peer, y_peer, partner):
        pl.semaphore_signal(barrier, inc=1, device_id=(peer,), device_id_type=pl.DeviceIdType.MESH)
    pl.semaphore_wait(barrier, 3)

    def remote(array, which):
        shard, out = ins[array], outs[array]
        source, slot, peer = {
            OWN_X0: (shard.at[0], 2 * me, x_peer), OWN_X1: (shard.at[1], 2 * me + 1, x_peer),
            OWN_Y0: (shard.at[0], 2 * me, y_peer), OWN_Y1: (shard.at[1], 2 * me + 1, y_peer),
            FORWARD_X: (None, 2 * y_peer + 1, x_peer), FORWARD_Y: (None, 2 * x_peer, y_peer),
            PARTNER_OWN: (shard, None, partner),
            PARTNER_X0: (None, 2 * x_peer, partner), PARTNER_X1: (None, 2 * x_peer + 1, partner),
            PARTNER_Y0: (None, 2 * y_peer, partner), PARTNER_Y1: (None, 2 * y_peer + 1, partner),
            PARTNER_D0: (None, 2 * diagonal, partner), PARTNER_D1: (None, 2 * diagonal + 1, partner)}[which]
        target = out.at[pl.ds(2 * me, 2)] if slot is None else out.at[slot]
        return pltpu.make_async_remote_copy(
            src_ref=target if source is None else source, dst_ref=target,
            send_sem=send_sem.at[array, which], recv_sem=recv_sem.at[array, which],
            device_id=(peer,), device_id_type=pl.DeviceIdType.MESH)

    def local(array):
        return pltpu.make_async_copy(ins[array], outs[array].at[pl.ds(2 * me, 2)], local_sem.at[array])

    def send_own(array):
        for which in (OWN_X0, OWN_Y1, PARTNER_OWN, OWN_X1, OWN_Y0):
            remote(array, which).start()
        local(array).start()

    def on_arrival(array, arrived, *then):
        remote(array, arrived).wait_recv()
        for which in then:
            remote(array, which).start()

    def first_halves(array):
        on_arrival(array, OWN_X0, FORWARD_Y, PARTNER_X0)
        on_arrival(array, OWN_Y1, FORWARD_X, PARTNER_Y1)

    def second_halves(array):
        on_arrival(array, OWN_X1, PARTNER_X1)
        on_arrival(array, OWN_Y0, PARTNER_Y0)

    def diagonals(array):
        on_arrival(array, FORWARD_X, PARTNER_D1)
        on_arrival(array, FORWARD_Y, PARTNER_D0)

    send_own(0)
    for array in range(count):
        first_halves(array)
        if array + 1 < count:
            send_own(array + 1)
        second_halves(array)
        if array > 0:
            diagonals(array - 1)
    diagonals(count - 1)
    for array in range(count):
        for which in range(PARTNER_OWN, COPIES):
            remote(array, which).wait_recv()
        for which in range(COPIES):
            remote(array, which).wait_send()
        local(array).wait()


def gather_now(*shards):
    count = len(shards)
    halves = [s.reshape(2, s.shape[0] // 2, s.shape[1]) for s in shards]
    outs = pl.pallas_call(
        functools.partial(gather_kernel, count), name="gather_now",
        in_specs=[pl.BlockSpec(memory_space=pltpu.VMEM)] * count,
        out_specs=[pl.BlockSpec(memory_space=pltpu.HBM)] * count,
        out_shape=[jax.ShapeDtypeStruct((16,) + h.shape[1:], h.dtype) for h in halves],
        scratch_shapes=[pltpu.SemaphoreType.DMA((count, COPIES)), pltpu.SemaphoreType.DMA((count, COPIES)),
                        pltpu.SemaphoreType.DMA((count,))],
        cost_estimate=pl.CostEstimate(flops=50 * 10 ** 9, bytes_accessed=10 ** 7, transcendentals=0),
        compiler_params=pltpu.CompilerParams(collective_id=1, has_side_effects=True))(*halves)
    return [o.reshape(8 * s.shape[0], s.shape[1]) for o, s in zip(outs, shards)]


def layer_norm_fwd(values, gain, bias):
    mean_val = jnp.mean(values, axis=-1, keepdims=True)
    centered = values - mean_val
    inv_std = lax.rsqrt(jnp.mean(centered * centered, axis=-1, keepdims=True) + LN_EPS)
    x_hat = centered * inv_std
    return x_hat * gain + bias, x_hat, inv_std


def layer_norm_bwd(grad_norm, x_hat, inv_std, gain):
    grad_hat = grad_norm * gain
    grad_vals = inv_std * (grad_hat - jnp.mean(grad_hat, axis=-1, keepdims=True)
                           - x_hat * jnp.mean(grad_hat * x_hat, axis=-1, keepdims=True))
    return grad_vals, jnp.sum(grad_norm * x_hat, axis=(0, 1)), jnp.sum(grad_norm, axis=(0, 1))


def einsum(spec, lhs, rhs):
    return jnp.einsum(spec, lhs, rhs, preferred_element_type=F32)


def flip(value, bit):
    return lax.ppermute(value, "fsdp", [(d, d ^ bit) for d in range(8)])


def pick(value, index):
    return lax.dynamic_index_in_dim(value, index, 0, keepdims=False).astype(F32)


def after(value, *done):
    return lax.optimization_barrier((value,) + done)[0]


def held(kept, *done):
    keep_a, keep_b = lax.optimization_barrier((kept[0], kept[1]) + done)[:2]
    return keep_a, keep_b, kept[2], kept[3]


def cross_first(name, kept, pos):
    keep_a, keep_b, send_a, send_b = kept
    y, x = pos[0], pos[1]
    with jax.named_scope(name + "_cross_one"):
        recv_a, recv_b = flip(send_a, X_BIT), flip(send_b, Y_BIT)
    next_a = (pick(keep_a, 1 - y) + pick(recv_a, 1 - y)).astype(BF16)
    next_b = (pick(keep_b, 1 - x) + pick(recv_b, 1 - x)).astype(BF16)
    return next_a, next_b, keep_a, keep_b, recv_a, recv_b


def cross_second(name, state):
    with jax.named_scope(name + "_cross_two"):
        return flip(state[0], Y_BIT), flip(state[1], X_BIT)


def cross_sum(state, last, pos, *done):
    keep_a, keep_b = lax.optimization_barrier((state[2], state[3]) + done)[:2]
    recv_a, recv_b, last_a, last_b = state[4:] + last
    y, x = pos[0], pos[1]
    return (pick(keep_a, y) + pick(recv_a, y) + last_a.astype(F32),
            pick(keep_b, x) + pick(recv_b, x) + last_b.astype(F32))


def token_major(value, *done):
    return lax.optimization_barrier(jnp.swapaxes(after(value, *done), 0, 1))


def finish_cols(sum_a, sum_b, pos):
    core = pos[2]
    mine = jnp.where(core == 0, sum_a, sum_b)
    other = flip(jnp.where(core == 0, sum_b, sum_a), CORE_BIT)
    return jnp.where(core == 0, jnp.concatenate([mine, other], axis=1), jnp.concatenate([other, mine], axis=1))


def sum_kernel(n, in_ref, out_ref, recv, send_sem, recv_sem):
    me = lax.axis_index("fsdp")
    barrier = pltpu.get_barrier_semaphore()
    peers = [lax.rem(me + step, n) for step in range(1, n)]
    for peer in peers:
        pl.semaphore_signal(barrier, inc=1, device_id=(peer,), device_id_type=pl.DeviceIdType.MESH)
    pl.semaphore_wait(barrier, n - 1)
    copies = []
    for step, peer in enumerate(peers):
        copies.append(pltpu.make_async_remote_copy(
            src_ref=in_ref.at[peer], dst_ref=recv.at[step], send_sem=send_sem.at[step], recv_sem=recv_sem.at[step],
            device_id=(peer,), device_id_type=pl.DeviceIdType.MESH))
        copies[-1].start()
    total = in_ref[me]
    for step, copy in enumerate(copies):
        copy.wait()
        total += recv[step]
    out_ref[...] = total


def sum_scatter(values):
    n, rows, cols = values.shape
    return pl.pallas_call(
        functools.partial(sum_kernel, n), name="sum_scatter",
        in_specs=[pl.BlockSpec(memory_space=pltpu.VMEM)], out_specs=pl.BlockSpec(memory_space=pltpu.VMEM),
        out_shape=jax.ShapeDtypeStruct((rows, cols), F32),
        scratch_shapes=[pltpu.VMEM((n - 1, rows, cols), F32), pltpu.SemaphoreType.DMA((n - 1,)),
                        pltpu.SemaphoreType.DMA((n - 1,))],
        cost_estimate=pl.CostEstimate(flops=4 * 10 ** 9, bytes_accessed=10 ** 6, transcendentals=0),
        compiler_params=pltpu.CompilerParams(collective_id=0, has_side_effects=True))(values)


def solution(mesh):
    specs = (P("fsdp"),) * 14
    n = mesh.shape["fsdp"]

    def gather(shard):
        return lax.all_gather(shard.astype(BF16), "fsdp", axis=0, tiled=True)

    def device_step(resid_in, grad_out, ln1_gain, ln1_bias, qkv_weight, qkv_bias, out_weight, out_bias,
                    ln2_gain, ln2_bias, fc_weight, fc_bias, proj_weight, proj_bias):
        vectors = (ln1_gain, ln1_bias, qkv_bias, out_bias, ln2_gain, ln2_bias, fc_bias, proj_bias)
        pieces, filled = [], 0
        for vec in vectors:
            pieces += [vec, jnp.zeros((-vec.shape[0] % 128,), F32)]
            filled += -(-vec.shape[0] // 128) * 128
        pieces.append(jnp.zeros((4096 - filled,), F32))
        packed = lax.reduce_precision(jnp.concatenate(pieces), 8, 7).reshape(32, 128)
        packed, qkv_weight, out_weight = gather_now(packed, qkv_weight.astype(BF16), out_weight.astype(BF16))
        fc_weight, proj_weight = [gather(after(w, packed)) for w in (fc_weight, proj_weight)]
        packed = lax.optimization_barrier(packed).reshape(n, 32, 128)
        full, at = [], 0
        for vec in vectors:
            count = -(-vec.shape[0] // 128)
            full.append(packed[:, at:at + count].reshape(n, count * 128)[:, :vec.shape[0]].reshape(-1))
            at += count
        ln1_gain, ln1_bias, qkv_bias, out_bias, ln2_gain, ln2_bias, fc_bias, proj_bias = [f.astype(F32) for f in full]

        resid = resid_in.astype(F32)
        normed, hat_one, inv_one = layer_norm_fwd(resid, ln1_gain, ln1_bias)
        normed_one = normed.astype(BF16)
        qkv = (einsum("bsw,wk->bsk", normed_one, qkv_weight) + qkv_bias).astype(BF16)
        mixed, lse = attn_fwd(qkv)
        middle = (resid + einsum("bsw,wv->bsv", mixed, out_weight) + out_bias).astype(BF16)
        middle_wide = middle.astype(F32)
        normed, hat_two, inv_two = layer_norm_fwd(middle_wide, ln2_gain, ln2_bias)
        normed_two = normed.astype(BF16)
        hidden, slope = fc_gelu(normed_two, fc_weight, fc_bias)

        device = lax.axis_index("fsdp")
        pos = jnp.stack([device // Y_BIT, (device // X_BIT) % 2, device % 2]).astype(jnp.int32)
        grad_wide = grad_out.astype(F32)
        d_proj_bias = jnp.sum(grad_wide, axis=(0, 1))
        proj_kept = wgrad(hidden, grad_out, WIDTH, True, 2)
        with jax.named_scope("dgrad_hidden"):
            grad_pre = einsum("bsw,fw->bsf", after(grad_out, *proj_kept[2:]), proj_weight) * slope
            grad_pre_low = grad_pre.astype(BF16)
        d_fc_bias = jnp.sum(grad_pre, axis=(0, 1))
        fc_kept = wgrad(normed_two, grad_pre_low, 1280, False, 3)
        proj_state = cross_first("proj", held(proj_kept, fc_kept[2]), pos)
        with jax.named_scope("dgrad_fc"):
            grad_norm = einsum("bsf,wf->bsw", after(grad_pre_low, *fc_kept[2:], *proj_state[:2]), fc_weight)
        grad_ln, d_ln2_gain, d_ln2_bias = layer_norm_bwd(grad_norm, hat_two, inv_two, ln2_gain)
        grad_middle = grad_wide + grad_ln
        proj_last = cross_second("proj", proj_state)
        grad_middle_low = grad_middle.astype(BF16)
        d_out_bias = jnp.sum(grad_middle, axis=(0, 1))
        out_kept = wgrad(mixed, grad_middle_low, 640, False, 4)
        with jax.named_scope("dgrad_out"):
            grad_mixed = einsum("bsv,wv->bsw", after(grad_middle_low, *out_kept[2:]), out_weight).astype(BF16)
        with jax.named_scope("attn_bwd_call"):
            grad_qkv, qkv_sums = attn_bwd(qkv, after(grad_mixed, *proj_last), lse)
        fc_state = cross_first("fc", held(fc_kept, qkv_sums), pos)
        out_state = cross_first("out", held(out_kept, qkv_sums), pos)
        d_qkv_bias = jnp.sum(qkv_sums, axis=(0, 1))
        fc_last, out_last = cross_second("fc", fc_state), cross_second("out", out_state)
        with jax.named_scope("dgrad_qkv"):
            grad_norm = einsum("bsk,wk->bsw", after(grad_qkv, *fc_state[:2], *out_state[:2]), qkv_weight)
        grad_ln, d_ln1_gain, d_ln1_bias = layer_norm_bwd(grad_norm, hat_one, inv_one, ln1_gain)
        grad_in = (grad_middle + grad_ln).astype(BF16)
        small = (d_ln1_gain, d_ln1_bias, d_qkv_bias, d_out_bias, d_ln2_gain, d_ln2_bias, d_fc_bias, d_proj_bias)
        rows = jnp.concatenate([s.reshape(n, -1) for s in small], axis=1)
        rows = jnp.pad(rows, ((0, 0), (0, 3072 - rows.shape[1])))
        rows = after(rows, *fc_last, *out_last)
        summed = sum_scatter(rows.reshape(n, 24, 128)).reshape(-1)
        qkv_kept = wgrad(normed_one, after(grad_qkv, summed), 1920, False, 5)
        tail_hidden = after(hidden, *qkv_kept[2:])
        with jax.named_scope("resid_product"):
            product = einsum("bsf,fw->bsw", tail_hidden, proj_weight)
        resid_out = (middle_wide + product + proj_bias).astype(BF16)
        qkv_state = cross_first("qkv", held(qkv_kept, resid_out), pos)
        qkv_last = cross_second("qkv", qkv_state)
        started = qkv_state[:2]
        resid_out, grad_in = token_major(resid_out, *started), token_major(grad_in, *started)
        d_proj_weight = jnp.concatenate(cross_sum(proj_state, proj_last, pos, *started), axis=1)
        d_fc_weight = finish_cols(*cross_sum(fc_state, fc_last, pos, *started), pos)
        d_out_weight = finish_cols(*cross_sum(out_state, out_last, pos, *started), pos)
        d_qkv_weight = finish_cols(*cross_sum(qkv_state, qkv_last, pos, resid_out, grad_in, d_proj_weight, d_fc_weight,
                                              d_out_weight), pos)
        resid_out, grad_in = jnp.swapaxes(resid_out, 0, 1), jnp.swapaxes(grad_in, 0, 1)

        shards, at = [], 0
        for vec in small:
            shards.append(summed[at:at + vec.shape[0] // n])
            at += vec.shape[0] // n
        (d_ln1_gain, d_ln1_bias, d_qkv_bias, d_out_bias, d_ln2_gain, d_ln2_bias, d_fc_bias, d_proj_bias) = shards
        return (resid_out, grad_in, d_ln1_gain, d_ln1_bias, d_qkv_weight, d_qkv_bias, d_out_weight, d_out_bias,
                d_ln2_gain, d_ln2_bias, d_fc_weight, d_fc_bias, d_proj_weight, d_proj_bias)

    return jax.shard_map(device_step, mesh=mesh, in_specs=specs, out_specs=specs, check_vma=False)
```
